32 devices in a mesh: ctx: 8 (over y, x, core), tp: 4 (over z).
Axes of the slice: x: 2, y: 2, z: 4, core: 2. Of those that a mesh axis runs over, the one named last changes fastest.
Arguments:
- hidden: bfloat16 [8, 8192], P(None, 'ctx'), may hold values from -4.8 to 4.8, as said below
- norm_gains: bfloat16 [4, 8192], P(None, 'ctx'), may hold values from 0.5 to 1.5
- w_query: bfloat16 [4, 8192, 8192], P(None, 'ctx', 'tp'), may hold values from -0.0625 to 0.0625
- w_key: bfloat16 [4, 8192, 1024], P(None, 'ctx', 'tp'), may hold values from -0.125 to 0.125
- w_value: bfloat16 [4, 8192, 1024], P(None, 'ctx', 'tp'), may hold values from -0.125 to 0.125
- w_out: bfloat16 [4, 8192, 8192], P(None, 'tp', 'ctx'), may hold values from -0.0625 to 0.0625
- key_cache: bfloat16 [4, 8, 8, 1024, 128], P(None, None, 'tp', 'ctx'), may hold values from -9 to 9
- value_cache: bfloat16 [4, 8, 8, 1024, 128], P(None, None, 'tp', 'ctx'), may hold values from -6 to 6
- lengths: int32 [8], replicated, may hold values from 1 to 1024, 4104 in all
Outputs:
- updated: float32 [8, 8192], P(None, 'ctx')
The draws below stay inside these ranges and needn't reach their ends.
Inputs may be any that keep to these rules, and one draw needn't show every extreme that they name: Each sequence has lengths[b] valid cache positions 0 .. lengths[b] - 1, between 1 and 1024; the longest sequence has exactly 1024; the new token sits at position lengths[b]. `hidden`: activations of order 0.2; in each block of 1024 consecutive features one sequence, chosen at random, has entries four times larger.
All inputs are finite; a program needn't handle non-finite values.
Results may differ from the reference program's by a relative error of at most 0.02.
Values sent between devices are 32-bit elements.
A program may use at most 128 MiB of HBM per device.

```python
import math
import jax
import jax.numpy as jnp
import numpy as np
from jax import lax

D = 8192
HQ = 64
KVH = 8
HD = 128
LAYERS = 4
BATCH = 8
CAP = 1024
D_DEV = 1024


def draw_hidden(key, part):
    base_key, owner_key = jax.random.split(jax.random.fold_in(key, 7))
    block_count = D // D_DEV
    owners = jax.random.randint(owner_key, (block_count,), 0, BATCH)
    column_owner = owners[jnp.arange(D) // D_DEV]
    factor = jnp.where(column_owner[None, :] == jnp.arange(BATCH)[:, None], 4.0, 1.0)
    base_draw = jnp.clip(jax.random.normal(base_key, (BATCH, D), jnp.float32), -6.0, 6.0)
    return (0.2 * factor * base_draw).astype(jnp.bfloat16)


def block_scale(rng, extent, pieces, smallest, high):
    gain = 1.0
    for axis_at, parts in pieces:
        draws = jax.random.uniform(jax.random.fold_in(jax.random.fold_in(rng, 6), axis_at), (parts,), jnp.float32, smallest / len(pieces), high / len(pieces))
        gain = gain * jnp.repeat(jnp.exp(draws), extent[axis_at] // parts).reshape((-1,) + (1,) * (len(extent) - 1 - axis_at))
    return gain


def profile(count, total, reach, slope):
    portions = [(1 << 20) // math.isqrt(grade ** slope) + 1 for grade in range(2, count + 1)]
    surplus, given = total - reach - (count - 1), [1] * (count - 1)
    while surplus > 0:
        movable = [i for i in range(count - 1) if given[i] < reach]
        mass, remaining = sum([portions[i] for i in movable]), surplus
        for i in movable:
            extra = min(reach - given[i], max(1, remaining * portions[i] // mass), surplus)
            given[i] = given[i] + extra
            surplus = surplus - extra
    return np.array([reach] + given)


def ragged(rng, amount, total, most, lean):
    if amount == 2:
        one = jax.random.randint(rng, (), max(1, total - most), min(most, total - 1) + 1)
        return jnp.stack([one, total - one])
    sizes = jnp.asarray(profile(amount, total, most, lean), jnp.int32)
    couples = (amount - 1) // 2
    source_of, taker = sizes[1:1 + 2 * couples:2], sizes[2:2 + 2 * couples:2]
    slack = jnp.minimum(source_of - 1, most - taker)
    shifted = jax.random.randint(jax.random.fold_in(rng, 1), (couples,), 0, 1 << 20) % (slack + 1)
    sizes = sizes.at[1:1 + 2 * couples:2].set(source_of - shifted).at[2:2 + 2 * couples:2].set(taker + shifted)
    return sizes[jax.random.permutation(jax.random.fold_in(rng, 2), amount)]


def scatter_about(stream_key, dims, scale, limit, pieces=(), kind=jnp.bfloat16):
    array = scale * jax.random.normal(stream_key, dims, jnp.float32)
    if pieces:
        array = array * block_scale(stream_key, dims, pieces, -0.22, 0.18)
    return jnp.clip(array, -limit, limit).astype(kind)


def setup_inputs(seed: int = 0) -> dict:
    key_list = jax.random.split(jax.random.key(seed), 10)
    hidden = draw_hidden(jax.random.fold_in(key_list[9], 71), 0)
    norm_gains = jnp.clip(1.0 + 0.1 * jax.random.normal(key_list[1], (LAYERS, D), jnp.float32), 0.5, 1.5).astype(jnp.bfloat16)
    w_query = scatter_about(key_list[2], (LAYERS, D, HQ * HD), D ** -0.5, 0.0625, ((1, 8), (2, 4)))
    w_key = scatter_about(key_list[3], (LAYERS, D, KVH * HD), (D // 4) ** -0.5, 0.125, ((1, 8), (2, 4)))
    w_value = scatter_about(key_list[4], (LAYERS, D, KVH * HD), (D // 4) ** -0.5, 0.125, ((1, 8), (2, 4)))
    w_out = scatter_about(key_list[5], (LAYERS, HQ * HD, D), (HQ * HD) ** -0.5, 0.0625, ((1, 4), (2, 8)))
    key_cache = scatter_about(key_list[6], (LAYERS, BATCH, KVH, CAP, HD), 1.5, 9.0, ((2, 4), (3, 8)))
    value_cache = scatter_about(key_list[7], (LAYERS, BATCH, KVH, CAP, HD), 1.0, 6.0, ((2, 4), (3, 8)))
    lengths = ragged(key_list[8], BATCH, BATCH * CAP // 2 + BATCH, CAP, 2).astype(jnp.int32)
    return dict(hidden=hidden, norm_gains=norm_gains, w_query=w_query, w_key=w_key, w_value=w_value, w_out=w_out, key_cache=key_cache, value_cache=value_cache, lengths=lengths)


mask_fill = -1e+30
norm_eps = 1e-05
rope_base = 500000.0

def rotate(vectors, positions):
    width = vectors.shape[-1]
    half_width = width // 2
    exponents = jnp.arange(half_width, dtype=jnp.float32) * (2.0 / width)
    frequency = jnp.exp(-exponents * math.log(rope_base))
    angles = positions.astype(jnp.float32)[:, None] * frequency[None, :]
    cosine = jnp.cos(angles)[:, None, :]
    sine_part = jnp.sin(angles)[:, None, :]
    first_half = vectors[..., :half_width]
    second_half = vectors[..., half_width:]
    return jnp.concatenate([first_half * cosine - second_half * sine_part, second_half * cosine + first_half * sine_part], axis=-1)

def reference(hidden, norm_gains, w_query, w_key, w_value, w_out, key_cache, value_cache, lengths):
    stream = hidden.astype(jnp.float32)
    group_size = HQ // KVH
    logit_multiplier = 1.0 / math.sqrt(HD)
    positions = jnp.arange(CAP, dtype=jnp.int32)
    usable = (positions[None, :] < lengths[:, None])[:, None, None, :]
    for layer_idx in range(LAYERS):
        reciprocal_value = lax.rsqrt(lax.optimization_barrier(jnp.sum(stream * stream, axis=1)) / D + norm_eps)
        scaled = (stream * norm_gains[layer_idx].astype(jnp.float32)).astype(jnp.bfloat16)
        raw_query = jnp.dot(scaled, w_query[layer_idx], preferred_element_type=jnp.float32)
        raw_key = jnp.dot(scaled, w_key[layer_idx], preferred_element_type=jnp.float32)
        raw_value = jnp.dot(scaled, w_value[layer_idx], preferred_element_type=jnp.float32)
        query = rotate((raw_query * reciprocal_value[:, None]).reshape(BATCH, HQ, HD), lengths).astype(jnp.bfloat16)
        fresh_lookup_vector = rotate((raw_key * reciprocal_value[:, None]).reshape(BATCH, KVH, HD), lengths).astype(jnp.bfloat16)
        new_value = (raw_value * reciprocal_value[:, None]).reshape(BATCH, KVH, HD).astype(jnp.bfloat16)
        shared_head_sets = query.reshape(BATCH, KVH, group_size, HD).astype(jnp.float32)
        scores = jnp.einsum('bkgd,bksd->bkgs', shared_head_sets, key_cache[layer_idx].astype(jnp.float32), precision=lax.Precision.HIGHEST) * logit_multiplier
        self_match_logit = jnp.einsum('uryj,urj->ury', shared_head_sets, fresh_lookup_vector.astype(jnp.float32), precision=lax.Precision.HIGHEST) * logit_multiplier
        masked = jnp.where(usable, scores, mask_fill)
        largest = jnp.maximum(lax.optimization_barrier(jnp.max(masked, axis=-1)), self_match_logit)
        attention_probabilities = jnp.where(usable, jnp.exp(masked - largest[..., None]), 0.0)
        fresh = jnp.exp(self_match_logit - largest)
        nearest_whole = lax.optimization_barrier(attention_probabilities.astype(jnp.bfloat16)).astype(jnp.float32)
        fresh_rounded = lax.optimization_barrier(fresh.astype(jnp.bfloat16)).astype(jnp.float32)
        numerator = jnp.einsum('bkgs,bksd->bkgd', nearest_whole, value_cache[layer_idx].astype(jnp.float32), precision=lax.Precision.HIGHEST)
        numerator = numerator + fresh_rounded[..., None] * new_value.astype(jnp.float32)[:, :, None, :]
        denominator = lax.optimization_barrier(jnp.sum(attention_probabilities, axis=-1)) + fresh
        context = (numerator / denominator[..., None]).reshape(BATCH, HQ * HD).astype(jnp.bfloat16)
        stream = stream + jnp.dot(context, w_out[layer_idx], preferred_element_type=jnp.float32)
    return stream
```

```python
import functools
import math

import jax
import jax.numpy as jnp
from jax import lax
from jax.experimental import pallas as pl
from jax.experimental.pallas import tpu as pltpu
from jax.sharding import PartitionSpec as P

mask_fill = -1e30
norm_eps = 1e-05
rope_base = 500000.0
MESH = pl.DeviceIdType.MESH


def kernel(dims, hidden_ref, gains_ref, lengths_ref, wq_h, wk_h, wv_h, wo_h, kc_h, vc_h, out_ref,
           wq, wk, wv, wo, kc, vc, gain, bias, cosine, sine, qp, qr, kvp, kvr, qf, qown, otmp, stmp,
           op, orr, cf, tps, tpr, w_sem, s_sem, r_sem, ts_sem, tr_sem):
    n, tn, layers, batch, feat, total, heads, kvl, hd, span = dims
    group = heads // kvl
    hpo = max(1, heads // n)
    owners = heads // hpo
    f32, bf16 = jnp.float32, jnp.bfloat16
    scale = 1.0 / math.sqrt(hd)
    me = lax.axis_index("ctx")
    mt = lax.axis_index("tp")
    weights = ((wq_h, wq), (wk_h, wk), (wv_h, wv), (kc_h, kc), (vc_h, vc), (wo_h, wo))

    def load(index, layer):
        source, target = weights[index]
        return pltpu.make_async_copy(source.at[layer], target.at[layer], w_sem.at[index, layer])

    for index in range(len(weights)):
        load(index, 0).start()

    peers = [lax.rem(me + r, n) for r in range(1, n)]
    tpeers = [lax.rem(mt + r, tn) for r in range(1, tn)]
    barrier = pltpu.get_barrier_semaphore()
    for p in peers:
        pl.semaphore_signal(barrier, inc=1, device_id={"ctx": p}, device_id_type=MESH)
    for p in tpeers:
        pl.semaphore_signal(barrier, inc=1, device_id={"tp": p}, device_id_type=MESH)

    row = lax.broadcasted_iota(jnp.int32, (batch, hd), 0)
    lane = lax.broadcasted_iota(jnp.int32, (batch, hd), 1)
    times = jnp.zeros((batch, hd), jnp.int32)
    slot = lax.broadcasted_iota(jnp.int32, (heads, span), 1) + me * span
    for b in range(batch):
        times = jnp.where(row == b, lengths_ref[b], times)
        bias[b * heads:(b + 1) * heads, :] = jnp.where(slot < lengths_ref[b], 0.0, mask_fill)
    half = hd // 2
    low = lane < half
    exponent = jnp.where(low, lane, lane - half).astype(f32) * (2.0 / hd)
    angle = times.astype(f32) * jnp.exp(-exponent * math.log(rope_base))
    cosine[...] = jnp.cos(angle)
    sine[...] = jnp.where(low, -jnp.sin(angle), jnp.sin(angle))
    for l in range(layers):
        gain[l] = jnp.broadcast_to(gains_ref[l:l + 1, :].astype(f32), (batch, feat))
    out_ref[...] = hidden_ref[...].astype(f32)

    pl.semaphore_wait(barrier, n - 1 + tn - 1)

    def rotate(u):
        return u * cosine[...] + pltpu.roll(u, half, 1) * sine[...]

    def rounded(u):
        return u.astype(bf16).astype(f32)

    def send(kind, r, source, target):
        return pltpu.make_async_remote_copy(
            src_ref=source, dst_ref=target, send_sem=s_sem.at[kind, r - 1],
            recv_sem=r_sem.at[kind, r - 1], device_id={"ctx": peers[r - 1]}, device_id_type=MESH)

    mine = lax.rem(me, owners)
    my_kv = (mine * hpo) // group
    rows = hpo * batch
    my_rows = pl.ds(pl.multiple_of(me * rows, rows), rows)
    width = hpo * hd

    def layer_step(l, carry):
        stream = out_ref[...]
        scaled = (stream * gain[l]).astype(bf16)
        squares = stream * stream
        fold = squares[:, 0:hd]
        for c in range(1, feat // hd):
            fold = fold + squares[:, c * hd:(c + 1) * hd]
        load(0, l).wait()

        @pl.when(l + 1 < layers)
        def _():
            for index in range(len(weights)):
                load(index, l + 1).start()

        q = jnp.dot(scaled, wq[l], preferred_element_type=f32)
        for i in range(owners):
            qp[i, :, 0:width] = q[:, i * width:(i + 1) * width]
            qp[i, :, width:width + hd] = fold
        qs = []
        for r in range(1, n):
            c = send(0, r, qp.at[lax.rem(peers[r - 1], owners)], qr.at[r - 1])
            c.start()
            qs.append(c)
        load(1, l).wait()
        load(2, l).wait()
        k = jnp.dot(scaled, wk[l], preferred_element_type=f32)
        v = jnp.dot(scaled, wv[l], preferred_element_type=f32)
        for j in range(kvl):
            kvp[j, :, 0:hd] = k[:, j * hd:(j + 1) * hd]
            kvp[j, :, hd:2 * hd] = v[:, j * hd:(j + 1) * hd]
        ks = []
        for r in range(1, n):
            owner = lax.rem(peers[r - 1], owners)
            c = send(1, r, kvp.at[(owner * hpo) // group], kvr.at[r - 1])
            c.start()
            ks.append(c)
        for c in qs:
            c.wait_recv()
        whole = qp[mine]
        for r in range(1, n):
            whole = whole + qr[r - 1]
        inverse = lax.rsqrt(jnp.sum(whole[:, width:width + hd], axis=1, keepdims=True) / total + norm_eps)
        for t in range(hpo):
            u = rotate(whole[:, t * hd:(t + 1) * hd] * inverse)
            qown[t] = rounded(u)
            qf[pl.ds(pl.multiple_of(me * rows + t * batch, batch), batch), :] = u
        gs = []
        for r in range(1, n):
            c = send(2, r, qf.at[my_rows], qf.at[my_rows])
            c.start()
            gs.append(c)
        for c in ks:
            c.wait_recv()
        kv = kvp[my_kv]
        for r in range(1, n):
            kv = kv + kvr[r - 1]
        new_key = rounded(rotate(kv[:, 0:hd] * inverse))
        new_value = rounded(kv[:, hd:2 * hd] * inverse)
        own = [jnp.sum(qown[t] * new_key, axis=1, keepdims=True) * scale for t in range(hpo)]
        load(3, l).wait()
        load(4, l).wait()
        for c in gs:
            c.wait_recv()
        scores = []
        for b in range(batch):
            qb = qf[pl.ds(b, heads, stride=batch), :].astype(bf16)
            for j in range(kvl):
                scores.append(lax.dot_general(
                    qb[j * group:(j + 1) * group], kc[l, b, j], (((1,), (1,)), ((), ())),
                    preferred_element_type=f32))
        masked = jnp.concatenate(scores, axis=0) * scale + bias[...]
        top = jnp.max(masked, axis=1, keepdims=True)
        weight = jnp.exp(masked - top)
        weight_sum = jnp.sum(weight, axis=1, keepdims=True)
        narrow = weight.astype(bf16)
        lanes = lax.broadcasted_iota(jnp.int32, (batch * heads, hd), 1)
        stmp[...] = jnp.where(lax.rem(lanes, 2) == 0, top, weight_sum)
        for b in range(batch):
            for j in range(kvl):
                at = b * heads + j * group
                otmp[at:at + group, :] = jnp.dot(narrow[at:at + group], vc[l, b, j], preferred_element_type=f32)
        for c in qs + ks + gs:
            c.wait_send()
        for i in range(owners):
            stat = None
            for t in range(hpo):
                h = i * hpo + t
                op[i, t * batch:(t + 1) * batch, :] = otmp[pl.ds(h, batch, stride=heads), :]
                piece = stmp[pl.ds(h, batch, stride=heads), :]
                stat = piece if stat is None else jnp.where(lane < 2 * t, stat, piece)
            op[i, rows:rows + batch, :] = stat
        os_ = []
        for r in range(1, n):
            c = send(3, r, op.at[lax.rem(peers[r - 1], owners)], orr.at[r - 1])
            c.start()
            os_.append(c)
        for c in os_:
            c.wait_recv()
        parts = [op[mine]] + [orr[r - 1] for r in range(1, n)]
        for t in range(hpo):
            tops = [part[rows:rows + batch, 2 * t:2 * t + 1] for part in parts]
            sums = [part[rows:rows + batch, 2 * t + 1:2 * t + 2] for part in parts]
            largest = own[t]
            for x in tops:
                largest = jnp.maximum(largest, x)
            fresh = jnp.exp(own[t] - largest)
            numerator = rounded(fresh) * new_value
            denominator = fresh
            for x, s, part in zip(tops, sums, parts):
                factor = jnp.exp(x - largest)
                denominator = denominator + s * factor
                numerator = numerator + part[t * batch:(t + 1) * batch, :] * factor
            cf[pl.ds(pl.multiple_of(me, 1), 1), :, t * hd:(t + 1) * hd] = (numerator / denominator)[None]
        cs = []
        for r in range(1, n):
            c = send(4, r, cf.at[me], cf.at[me])
            c.start()
            cs.append(c)
        load(5, l).wait()
        for c in cs:
            c.wait_recv()
        context = jnp.concatenate([cf[i] for i in range(owners)], axis=1).astype(bf16)
        part = jnp.dot(context, wo[l], preferred_element_type=f32)
        odd = lax.rem(l, 2)
        tps[...] = part
        ts = []
        for r in range(1, tn):
            c = pltpu.make_async_remote_copy(
                src_ref=tps, dst_ref=tpr.at[odd, r - 1], send_sem=ts_sem.at[r - 1],
                recv_sem=tr_sem.at[odd, r - 1], device_id={"tp": tpeers[r - 1]}, device_id_type=MESH)
            c.start()
            ts.append(c)
        for c in os_ + cs:
            c.wait_send()
        stream = stream + part
        for r, c in enumerate(ts):
            c.wait_recv()
            stream = stream + tpr[odd, r]
        out_ref[...] = stream
        for c in ts:
            c.wait_send()
        return carry

    lax.fori_loop(0, layers, layer_step, 0)


def shards(sizes, hidden, norm_gains, w_query, w_key, w_value, w_out, key_cache, value_cache, lengths):
    n, tn = sizes
    layers, feat, columns = w_query.shape
    batch = hidden.shape[0]
    _, _, kvl, span, hd = key_cache.shape
    heads = columns // hd
    hpo = max(1, heads // n)
    owners = heads // hpo
    dims = (n, tn, layers, batch, feat, feat * n, heads, kvl, hd, span)
    f32 = jnp.float32
    vmem = pl.BlockSpec(memory_space=pltpu.VMEM)
    far = pl.BlockSpec(memory_space=pl.ANY)

    def like(array):
        return pltpu.VMEM(array.shape, array.dtype)

    return pl.pallas_call(
        functools.partial(kernel, dims),
        out_shape=jax.ShapeDtypeStruct((batch, feat), f32),
        in_specs=[vmem, vmem, pl.BlockSpec(memory_space=pltpu.SMEM)] + [far] * 6,
        out_specs=vmem,
        scratch_shapes=[
            like(w_query), like(w_key), like(w_value), like(w_out), like(key_cache), like(value_cache),
            pltpu.VMEM((layers, batch, feat), f32),
            pltpu.VMEM((batch * heads, span), f32),
            pltpu.VMEM((batch, hd), f32),
            pltpu.VMEM((batch, hd), f32),
            pltpu.VMEM((owners, batch, hpo * hd + hd), f32),
            pltpu.VMEM((n - 1, batch, hpo * hd + hd), f32),
            pltpu.VMEM((kvl, batch, 2 * hd), f32),
            pltpu.VMEM((n - 1, batch, 2 * hd), f32),
            pltpu.VMEM((n * hpo * batch, hd), f32),
            pltpu.VMEM((hpo, batch, hd), f32),
            pltpu.VMEM((batch * heads, hd), f32),
            pltpu.VMEM((batch * heads, hd), f32),
            pltpu.VMEM((owners, hpo * batch + batch, hd), f32),
            pltpu.VMEM((n - 1, hpo * batch + batch, hd), f32),
            pltpu.VMEM((n, batch, hpo * hd), f32),
            pltpu.VMEM((batch, feat), f32),
            pltpu.VMEM((2, tn - 1, batch, feat), f32),
            pltpu.SemaphoreType.DMA((6, layers)),
            pltpu.SemaphoreType.DMA((5, n - 1)),
            pltpu.SemaphoreType.DMA((5, n - 1)),
            pltpu.SemaphoreType.DMA((tn - 1,)),
            pltpu.SemaphoreType.DMA((2, tn - 1)),
        ],
        compiler_params=pltpu.CompilerParams(
            collective_id=0, has_side_effects=True, vmem_limit_bytes=60 * 1024 * 1024),
    )(hidden, norm_gains, lengths, w_query, w_key, w_value, w_out, key_cache, value_cache)


def solution(mesh):
    sizes = (mesh.shape["ctx"], mesh.shape["tp"])
    return jax.shard_map(
        functools.partial(shards, sizes),
        mesh=mesh,
        in_specs=(
            P(None, "ctx"),
            P(None, "ctx"),
            P(None, "ctx", "tp"),
            P(None, "ctx", "tp"),
            P(None, "ctx", "tp"),
            P(None, "tp", "ctx"),
            P(None, None, "tp", "ctx", None),
            P(None, None, "tp", "ctx", None),
            P(),
        ),
        out_specs=P(None, "ctx"),
        check_vma=False,
    )
```

```python
import functools
import math

import jax
import jax.numpy as jnp
from jax import lax
from jax.experimental import pallas as pl
from jax.experimental.pallas import tpu as pltpu
from jax.sharding import PartitionSpec as P

mask_fill = -1e30
norm_eps = 1e-05
rope_base = 500000.0
MESH = pl.DeviceIdType.MESH


def kernel(dims, hidden_ref, gains_ref, lengths_ref, wq_h, wk_h, wv_h, wo_h, kc_h, vc_h, out_ref,
           wq, wk, wv, wo, kc, vc, gain, bias, cosine, sine, qp, qr, kvp, kvr, qf, qown, otmp, stmp,
           op, orr, cf, tps, tpr, w_sem, s_sem, r_sem, ts_sem, tr_sem):
    n, tn, layers, batch, feat, total, heads, kvl, hd, span = dims
    group = heads // kvl
    hpo = max(1, heads // n)
    owners = heads // hpo
    f32, bf16 = jnp.float32, jnp.bfloat16
    pieces = tps.shape[0]
    piece = feat // pieces
    scale = 1.0 / math.sqrt(hd)
    me = lax.axis_index("ctx")
    mt = lax.axis_index("tp")
    weights = ((wq_h, wq), (wk_h, wk), (wv_h, wv), (kc_h, kc), (vc_h, vc), (wo_h, wo))

    def load(index, layer):
        source, target = weights[index]
        return pltpu.make_async_copy(source.at[layer], target.at[layer], w_sem.at[index, layer])

    for index in range(len(weights)):
        load(index, 0).start()

    peers = [lax.rem(me + r, n) for r in range(1, n)]
    tpeers = [lax.rem(mt + r, tn) for r in range(1, tn)]
    barrier = pltpu.get_barrier_semaphore()
    for p in peers:
        pl.semaphore_signal(barrier, inc=1, device_id={"ctx": p}, device_id_type=MESH)
    for p in tpeers:
        pl.semaphore_signal(barrier, inc=1, device_id={"tp": p}, device_id_type=MESH)

    row = lax.broadcasted_iota(jnp.int32, (batch, hd), 0)
    lane = lax.broadcasted_iota(jnp.int32, (batch, hd), 1)
    times = jnp.zeros((batch, hd), jnp.int32)
    slot = lax.broadcasted_iota(jnp.int32, (heads, span), 1) + me * span
    for b in range(batch):
        times = jnp.where(row == b, lengths_ref[b], times)
        bias[b * heads:(b + 1) * heads, :] = jnp.where(slot < lengths_ref[b], 0.0, mask_fill)
    half = hd // 2
    low = lane < half
    exponent = jnp.where(low, lane, lane - half).astype(f32) * (2.0 / hd)
    angle = times.astype(f32) * jnp.exp(-exponent * math.log(rope_base))
    cosine[...] = jnp.cos(angle)
    sine[...] = jnp.where(low, -jnp.sin(angle), jnp.sin(angle))
    for l in range(layers):
        gain[l] = jnp.broadcast_to(gains_ref[l:l + 1, :].astype(f32), (batch, feat))
    out_ref[...] = hidden_ref[...].astype(f32)

    pl.semaphore_wait(barrier, n - 1 + tn - 1)

    def rotate(u):
        return u * cosine[...] + pltpu.roll(u, half, 1) * sine[...]

    def rounded(u):
        return u.astype(bf16).astype(f32)

    def send(kind, r, source, target):
        return pltpu.make_async_remote_copy(
            src_ref=source, dst_ref=target, send_sem=s_sem.at[kind, r - 1],
            recv_sem=r_sem.at[kind, r - 1], device_id={"ctx": peers[r - 1]}, device_id_type=MESH)

    order = sorted(range(1, n), key=lambda r: (-min(r, n - r), r))
    mine = lax.rem(me, owners)
    my_kv = (mine * hpo) // group
    rows = hpo * batch
    my_rows = pl.ds(pl.multiple_of(me * rows, rows), rows)
    width = hpo * hd

    def layer_step(l, carry):
        stream = out_ref[...]
        scaled = (stream * gain[l]).astype(bf16)
        squares = stream * stream
        fold = squares[:, 0:hd]
        for c in range(1, feat // hd):
            fold = fold + squares[:, c * hd:(c + 1) * hd]
        load(0, l).wait()

        @pl.when(l + 1 < layers)
        def _():
            for index in range(len(weights)):
                load(index, l + 1).start()

        q = jnp.dot(scaled, wq[l], preferred_element_type=f32)
        for i in range(owners):
            qp[i, :, 0:width] = q[:, i * width:(i + 1) * width]
            qp[i, :, width:width + hd] = fold
        qs = []
        for r in order:
            c = send(0, r, qp.at[lax.rem(peers[r - 1], owners)], qr.at[r - 1])
            c.start()
            qs.append(c)
        load(1, l).wait()
        load(2, l).wait()
        k = jnp.dot(scaled, wk[l], preferred_element_type=f32)
        v = jnp.dot(scaled, wv[l], preferred_element_type=f32)
        for j in range(kvl):
            kvp[j, :, 0:hd] = k[:, j * hd:(j + 1) * hd]
            kvp[j, :, hd:2 * hd] = v[:, j * hd:(j + 1) * hd]
        ks = []
        for r in order:
            owner = lax.rem(peers[r - 1], owners)
            c = send(1, r, kvp.at[(owner * hpo) // group], kvr.at[r - 1])
            c.start()
            ks.append(c)
        for c in qs:
            c.wait_recv()
        whole = qp[mine]
        for r in range(1, n):
            whole = whole + qr[r - 1]
        inverse = lax.rsqrt(jnp.sum(whole[:, width:width + hd], axis=1, keepdims=True) / total + norm_eps)
        for t in range(hpo):
            u = rotate(whole[:, t * hd:(t + 1) * hd] * inverse)
            qown[t] = rounded(u)
            qf[pl.ds(pl.multiple_of(me * rows + t * batch, batch), batch), :] = u
        gs = []
        for r in order:
            c = send(2, r, qf.at[my_rows], qf.at[my_rows])
            c.start()
            gs.append(c)
        for c in ks:
            c.wait_recv()
        kv = kvp[my_kv]
        for r in range(1, n):
            kv = kv + kvr[r - 1]
        new_key = rounded(rotate(kv[:, 0:hd] * inverse))
        new_value = rounded(kv[:, hd:2 * hd] * inverse)
        own = [jnp.sum(qown[t] * new_key, axis=1, keepdims=True) * scale for t in range(hpo)]
        load(3, l).wait()
        load(4, l).wait()
        for c in gs:
            c.wait_recv()
        scores = []
        for b in range(batch):
            qb = qf[pl.ds(b, heads, stride=batch), :].astype(bf16)
            for j in range(kvl):
                scores.append(lax.dot_general(
                    qb[j * group:(j + 1) * group], kc[l, b, j], (((1,), (1,)), ((), ())),
                    preferred_element_type=f32))
        masked = jnp.concatenate(scores, axis=0) * scale + bias[...]
        top = jnp.max(masked, axis=1, keepdims=True)
        weight = jnp.exp(masked - top)
        weight_sum = jnp.sum(weight, axis=1, keepdims=True)
        narrow = weight.astype(bf16)
        lanes = lax.broadcasted_iota(jnp.int32, (batch * heads, hd), 1)
        stmp[...] = jnp.where(lax.rem(lanes, 2) == 0, top, weight_sum)
        for b in range(batch):
            for j in range(kvl):
                at = b * heads + j * group
                otmp[at:at + group, :] = jnp.dot(narrow[at:at + group], vc[l, b, j], preferred_element_type=f32)
        for c in qs + ks + gs:
            c.wait_send()
        for i in range(owners):
            stat = None
            for t in range(hpo):
                h = i * hpo + t
                op[i, t * batch:(t + 1) * batch, :] = otmp[pl.ds(h, batch, stride=heads), :]
                tile = stmp[pl.ds(h, batch, stride=heads), :]
                stat = tile if stat is None else jnp.where(lane < 2 * t, stat, tile)
            op[i, rows:rows + batch, :] = stat
        os_ = []
        for r in order:
            c = send(3, r, op.at[lax.rem(peers[r - 1], owners)], orr.at[r - 1])
            c.start()
            os_.append(c)
        for c in os_:
            c.wait_recv()
        parts = [op[mine]] + [orr[r - 1] for r in range(1, n)]
        for t in range(hpo):
            tops = [part[rows:rows + batch, 2 * t:2 * t + 1] for part in parts]
            sums = [part[rows:rows + batch, 2 * t + 1:2 * t + 2] for part in parts]
            largest = own[t]
            for x in tops:
                largest = jnp.maximum(largest, x)
            fresh = jnp.exp(own[t] - largest)
            numerator = rounded(fresh) * new_value
            denominator = fresh
            for x, s, part in zip(tops, sums, parts):
                factor = jnp.exp(x - largest)
                denominator = denominator + s * factor
                numerator = numerator + part[t * batch:(t + 1) * batch, :] * factor
            cf[pl.ds(pl.multiple_of(me, 1), 1), :, t * hd:(t + 1) * hd] = (numerator / denominator)[None]
        cs = []
        for r in order:
            c = send(4, r, cf.at[me], cf.at[me])
            c.start()
            cs.append(c)
        load(5, l).wait()
        for c in cs:
            c.wait_recv()
        context = jnp.concatenate([cf[i] for i in range(owners)], axis=1).astype(bf16)
        odd = lax.rem(l, 2)
        ts = []
        for g in range(pieces):
            cut = slice(g * piece, (g + 1) * piece)
            tps[g] = jnp.dot(context, wo[l, :, cut], preferred_element_type=f32)
            for r in range(1, tn):
                c = pltpu.make_async_remote_copy(
                    src_ref=tps.at[g], dst_ref=tpr.at[odd, g, r - 1], send_sem=ts_sem.at[g, r - 1],
                    recv_sem=tr_sem.at[odd, g, r - 1], device_id={"tp": tpeers[r - 1]}, device_id_type=MESH)
                c.start()
                ts.append(c)
        for c in os_ + cs:
            c.wait_send()
        for g in range(pieces):
            cut = slice(g * piece, (g + 1) * piece)
            moved = out_ref[:, cut] + tps[g]
            for r in range(1, tn):
                ts[g * (tn - 1) + r - 1].wait_recv()
                moved = moved + tpr[odd, g, r - 1]
            out_ref[:, cut] = moved
        for c in ts:
            c.wait_send()
        return carry

    lax.fori_loop(0, layers, layer_step, 0)


def shards(sizes, hidden, norm_gains, w_query, w_key, w_value, w_out, key_cache, value_cache, lengths):
    n, tn = sizes
    layers, feat, columns = w_query.shape
    batch = hidden.shape[0]
    _, _, kvl, span, hd = key_cache.shape
    heads = columns // hd
    hpo = max(1, heads // n)
    owners = heads // hpo
    dims = (n, tn, layers, batch, feat, feat * n, heads, kvl, hd, span)
    pieces = 2
    f32 = jnp.float32
    vmem = pl.BlockSpec(memory_space=pltpu.VMEM)
    far = pl.BlockSpec(memory_space=pl.ANY)

    def like(array):
        return pltpu.VMEM(array.shape, array.dtype)

    return pl.pallas_call(
        functools.partial(kernel, dims),
        out_shape=jax.ShapeDtypeStruct((batch, feat), f32),
        in_specs=[vmem, vmem, pl.BlockSpec(memory_space=pltpu.SMEM)] + [far] * 6,
        out_specs=vmem,
        scratch_shapes=[
            like(w_query), like(w_key), like(w_value), like(w_out), like(key_cache), like(value_cache),
            pltpu.VMEM((layers, batch, feat), f32),
            pltpu.VMEM((batch * heads, span), f32),
            pltpu.VMEM((batch, hd), f32),
            pltpu.VMEM((batch, hd), f32),
            pltpu.VMEM((owners, batch, hpo * hd + hd), f32),
            pltpu.VMEM((n - 1, batch, hpo * hd + hd), f32),
            pltpu.VMEM((kvl, batch, 2 * hd), f32),
            pltpu.VMEM((n - 1, batch, 2 * hd), f32),
            pltpu.VMEM((n * hpo * batch, hd), f32),
            pltpu.VMEM((hpo, batch, hd), f32),
            pltpu.VMEM((batch * heads, hd), f32),
            pltpu.VMEM((batch * heads, hd), f32),
            pltpu.VMEM((owners, hpo * batch + batch, hd), f32),
            pltpu.VMEM((n - 1, hpo * batch + batch, hd), f32),
            pltpu.VMEM((n, batch, hpo * hd), f32),
            pltpu.VMEM((pieces, batch, feat // pieces), f32),
            pltpu.VMEM((2, pieces, tn - 1, batch, feat // pieces), f32),
            pltpu.SemaphoreType.DMA((6, layers)),
            pltpu.SemaphoreType.DMA((5, n - 1)),
            pltpu.SemaphoreType.DMA((5, n - 1)),
            pltpu.SemaphoreType.DMA((pieces, tn - 1)),
            pltpu.SemaphoreType.DMA((2, pieces, tn - 1)),
        ],
        compiler_params=pltpu.CompilerParams(
            collective_id=0, has_side_effects=True, vmem_limit_bytes=60 * 1024 * 1024),
    )(hidden, norm_gains, lengths, w_query, w_key, w_value, w_out, key_cache, value_cache)


def solution(mesh):
    sizes = (mesh.shape["ctx"], mesh.shape["tp"])
    return jax.shard_map(
        functools.partial(shards, sizes),
        mesh=mesh,
        in_specs=(
            P(None, "ctx"),
            P(None, "ctx"),
            P(None, "ctx", "tp"),
            P(None, "ctx", "tp"),
            P(None, "ctx", "tp"),
            P(None, "tp", "ctx"),
            P(None, None, "tp", "ctx", None),
            P(None, None, "tp", "ctx", None),
            P(),
        ),
        out_specs=P(None, "ctx"),
        check_vma=False,
    )
```
